8 devices in a mesh: dp: 1 (over z), kv: 8 (over y, x, core).
Axes of the slice: x: 2, y: 2, z: 1, core: 2. Of those that a mesh axis runs over, the one named last changes fastest.
Arguments:
- x_first: bfloat16 [16, 1024], P('dp')
- next_emb: bfloat16 [2, 16, 1024], P(None, 'dp')
- k_cache: bfloat16 [16, 2048, 8, 64], P('dp', 'kv')
- v_cache: bfloat16 [16, 2048, 8, 64], P('dp', 'kv')
- seq_len: int32 [16], P('dp')
- ln1_gain: float32 [1024], replicated
- ln1_bias: float32 [1024], replicated
- w_q: bfloat16 [1024, 1024], replicated
- b_q: float32 [1024], replicated
- w_k: bfloat16 [1024, 512], replicated
- b_k: float32 [512], replicated
- w_v: bfloat16 [1024, 512], replicated
- b_v: float32 [512], replicated
- w_o: bfloat16 [1024, 1024], replicated
- b_o: float32 [1024], replicated
- ln2_gain: float32 [1024], replicated
- ln2_bias: float32 [1024], replicated
- w_router: bfloat16 [1024, 32], replicated
- w_gate: bfloat16 [32, 1024, 512], P(None, None, 'kv')
- w_up: bfloat16 [32, 1024, 512], P(None, None, 'kv')
- w_down: bfloat16 [32, 512, 1024], P(None, 'kv')
- long_factor: float32 [32], replicated
- expert_idx: int32 [3, 16, 8], P(None, 'dp')
- route_mask: int32 [3, 16, 8, 32], P(None, 'dp')
Outputs:
- output 1: bfloat16 [3, 16, 1024], P(None, 'dp')
- output 2: bfloat16 [16, 3, 8, 64], P('dp')
- output 3: bfloat16 [16, 3, 8, 64], P('dp')
All inputs are finite; a program needn't handle non-finite values.
Results may differ from the reference program's by a relative error of at most 0.0124876.
Values sent between devices are 32-bit elements.
A program may use at most 1 GiB of HBM per device.

```python
import math
import jax
import jax.numpy as jnp
from jax import lax

BATCH_SIZE = 16
SHARD_LEN = 256
KV_GROUP = 8
CACHE_LEN = 2048
D_MODEL = 1024
Q_HEADS = 16
KV_HEADS = 8
HEAD_DIM = 64
NUM_EXPERTS = 32
TOP_K = 8
FF_DIM = 512
NUM_STEPS = 3
SEG_COUNT = 64

HALF_DIM = HEAD_DIM // 2
Q_GROUP = Q_HEADS // KV_HEADS
FF_SHARD = FF_DIM // KV_GROUP
ROPE_BASE = 10000.0
ROPE_MSCALE = math.sqrt(1.0 + math.log(32.0) / math.log(4096.0))
NORM_EPS = 1e-5
NEG_FILL = -1e30


def setup_inputs(seed: int = 0, part: int = 0) -> dict:
    base_key = jax.random.key(seed)
    shared_keys = jax.random.split(base_key, 17)
    part_keys = jax.random.split(jax.random.fold_in(base_key, part), 9)
    q_width = Q_HEADS * HEAD_DIM
    kv_width = KV_HEADS * HEAD_DIM
    d_scale = D_MODEL ** -0.5

    def normal(rand_key, arr_dims, factor):
        return jax.random.normal(rand_key, arr_dims, jnp.float32) * factor

    x_first = normal(part_keys[0], (BATCH_SIZE, D_MODEL), 1.0).astype(jnp.bfloat16)
    next_emb = normal(part_keys[1], (NUM_STEPS - 1, BATCH_SIZE, D_MODEL), 1.0).astype(jnp.bfloat16)
    seg_index = (jnp.arange(CACHE_LEN) * SEG_COUNT) // CACHE_LEN
    key_segs = normal(part_keys[2], (BATCH_SIZE, SEG_COUNT, KV_HEADS, HEAD_DIM), 1.0)
    value_segs = normal(part_keys[3], (BATCH_SIZE, SEG_COUNT, KV_HEADS, HEAD_DIM), 4.0)
    cache_dims = (BATCH_SIZE, CACHE_LEN, KV_HEADS, HEAD_DIM)
    k_cache = (normal(part_keys[4], cache_dims, 1.0) + key_segs[:, seg_index]).astype(jnp.bfloat16)
    v_cache = (normal(part_keys[5], cache_dims, 1.0) + value_segs[:, seg_index]).astype(jnp.bfloat16)
    drawn_lens = jax.random.randint(part_keys[6], (BATCH_SIZE,), CACHE_LEN // 4, CACHE_LEN + 1)
    seq_len = jnp.where(jnp.arange(BATCH_SIZE) == 0, CACHE_LEN, drawn_lens).astype(jnp.int32)
    rank_scores = jax.random.randint(part_keys[7], (NUM_STEPS, BATCH_SIZE, NUM_EXPERTS), 0, 1 << 20)
    expert_order = jnp.argsort(rank_scores * NUM_EXPERTS + jnp.arange(NUM_EXPERTS), axis=-1)
    expert_idx = expert_order[..., :TOP_K].astype(jnp.int32)
    chosen = (expert_idx[..., None] == jnp.arange(NUM_EXPERTS)).astype(jnp.int32)
    earlier = jnp.cumsum(chosen, axis=2) - chosen
    coin_flip = jax.random.randint(part_keys[8], (NUM_STEPS, BATCH_SIZE, TOP_K, NUM_EXPERTS), 0, 2)
    route_mask = jnp.where(chosen == 1, 1, jnp.where(earlier > 0, 0, coin_flip)).astype(jnp.int32)
    return {
        'x_first': x_first,
        'next_emb': next_emb,
        'k_cache': k_cache,
        'v_cache': v_cache,
        'seq_len': seq_len,
        'ln1_gain': 1.0 + normal(shared_keys[0], (D_MODEL,), 0.3),
        'ln1_bias': normal(shared_keys[1], (D_MODEL,), 0.3),
        'w_q': normal(shared_keys[2], (D_MODEL, q_width), d_scale).astype(jnp.bfloat16),
        'b_q': normal(shared_keys[3], (q_width,), 0.5),
        'w_k': normal(shared_keys[4], (D_MODEL, kv_width), d_scale).astype(jnp.bfloat16),
        'b_k': normal(shared_keys[5], (kv_width,), 0.5),
        'w_v': normal(shared_keys[6], (D_MODEL, kv_width), d_scale).astype(jnp.bfloat16),
        'b_v': normal(shared_keys[7], (kv_width,), 0.5),
        'w_o': normal(shared_keys[8], (q_width, D_MODEL), q_width ** -0.5).astype(jnp.bfloat16),
        'b_o': normal(shared_keys[9], (D_MODEL,), 0.3),
        'ln2_gain': 1.0 + normal(shared_keys[10], (D_MODEL,), 0.3),
        'ln2_bias': normal(shared_keys[11], (D_MODEL,), 0.3),
        'w_router': normal(shared_keys[12], (D_MODEL, NUM_EXPERTS), 1.5 * d_scale).astype(jnp.bfloat16),
        'w_gate': normal(shared_keys[13], (NUM_EXPERTS, D_MODEL, FF_DIM), d_scale).astype(jnp.bfloat16),
        'w_up': normal(shared_keys[14], (NUM_EXPERTS, D_MODEL, FF_DIM), d_scale).astype(jnp.bfloat16),
        'w_down': normal(shared_keys[15], (NUM_EXPERTS, FF_DIM, D_MODEL), FF_DIM ** -0.5).astype(jnp.bfloat16),
        'long_factor': jnp.exp(jax.random.uniform(shared_keys[16], (HALF_DIM,), jnp.float32, 0.0, 3.5)),
        'expert_idx': expert_idx,
        'route_mask': route_mask,
    }


def layer_norm(x_in, gain_vec, bias_vec):
    x_f32 = x_in.astype(jnp.float32)
    mean_val = jnp.mean(x_f32, axis=-1, keepdims=True)
    centered = x_f32 - mean_val
    var_val = jnp.mean(centered * centered, axis=-1, keepdims=True)
    return (centered * lax.rsqrt(var_val + NORM_EPS) * gain_vec + bias_vec).astype(jnp.bfloat16)


def rotate_heads(x_in, angles):
    cos_half = jnp.cos(angles) * ROPE_MSCALE
    sin_half = jnp.sin(angles) * ROPE_MSCALE
    cos_full = jnp.concatenate([cos_half, cos_half], axis=-1)[:, None, :]
    sin_full = jnp.concatenate([sin_half, sin_half], axis=-1)[:, None, :]
    x_f32 = x_in.astype(jnp.float32)
    rotated = jnp.concatenate([-x_f32[..., HALF_DIM:], x_f32[..., :HALF_DIM]], axis=-1)
    return (x_f32 * cos_full + rotated * sin_full).astype(jnp.bfloat16)


def partial_stats(q_grp, keys, values, keep_mask):
    scores = jnp.einsum('bkgd,btkd->bkgt', q_grp.astype(jnp.float32), keys.astype(jnp.float32)) * (HEAD_DIM ** -0.5)
    keep_full = keep_mask[:, None, None, :]
    scores = jnp.where(keep_full, scores, NEG_FILL)
    run_max = jnp.max(scores, axis=-1)
    weights = jnp.where(keep_full, jnp.exp(scores - run_max[..., None]), 0.0)
    run_sum = jnp.sum(weights, axis=-1)
    out_part = jnp.einsum('bkgt,btkd->bkgd', weights.astype(jnp.bfloat16).astype(jnp.float32), values.astype(jnp.float32))
    return run_max, run_sum, out_part


def reference(x_first, next_emb, k_cache, v_cache, seq_len, ln1_gain, ln1_bias, w_q, b_q, w_k, b_k, w_v, b_v, w_o, b_o, ln2_gain, ln2_bias, w_router, w_gate, w_up, w_down, long_factor, expert_idx, route_mask):
    inv_freq = 1.0 / (long_factor * ROPE_BASE ** (jnp.arange(HALF_DIM, dtype=jnp.float32) * 2.0 / HEAD_DIM))
    step_inputs = jnp.concatenate([x_first[None], next_emb], axis=0)
    shard_ids = jnp.arange(KV_GROUP)
    tail_slots = jnp.arange(NUM_STEPS)

    def decode_step(step_carry, step_in):
        tail_k, tail_v = step_carry
        x_in, idx_step, mask_step, step_idx = step_in
        h_norm = layer_norm(x_in, ln1_gain, ln1_bias)
        q_new = (jnp.dot(h_norm, w_q, preferred_element_type=jnp.float32) + b_q).astype(jnp.bfloat16).reshape(BATCH_SIZE, Q_HEADS, HEAD_DIM)
        k_new = (jnp.dot(h_norm, w_k, preferred_element_type=jnp.float32) + b_k).astype(jnp.bfloat16).reshape(BATCH_SIZE, KV_HEADS, HEAD_DIM)
        v_new = (jnp.dot(h_norm, w_v, preferred_element_type=jnp.float32) + b_v).astype(jnp.bfloat16).reshape(BATCH_SIZE, KV_HEADS, HEAD_DIM)
        angles = (seq_len + step_idx).astype(jnp.float32)[:, None] * inv_freq[None, :]
        q_grp = rotate_heads(q_new, angles).reshape(BATCH_SIZE, KV_HEADS, Q_GROUP, HEAD_DIM)
        k_rot = rotate_heads(k_new, angles)
        tail_k = lax.dynamic_update_slice_in_dim(tail_k, k_rot[:, None], step_idx, axis=1)
        tail_v = lax.dynamic_update_slice_in_dim(tail_v, v_new[:, None], step_idx, axis=1)

        def one_shard(shard_id):
            k_blk = lax.dynamic_slice_in_dim(k_cache, shard_id * SHARD_LEN, SHARD_LEN, axis=1)
            v_blk = lax.dynamic_slice_in_dim(v_cache, shard_id * SHARD_LEN, SHARD_LEN, axis=1)
            positions = shard_id * SHARD_LEN + jnp.arange(SHARD_LEN)
            keep_mask = positions[None, :] < seq_len[:, None]
            return partial_stats(q_grp, k_blk, v_blk, keep_mask)

        cache_max, cache_sum, cache_out = lax.map(one_shard, shard_ids)
        tail_keep = jnp.broadcast_to(tail_slots[None, :] <= step_idx, (BATCH_SIZE, NUM_STEPS))
        tail_max, tail_sum, tail_out = partial_stats(q_grp, tail_k, tail_v, tail_keep)
        max_all = jnp.concatenate([cache_max, tail_max[None]], axis=0)
        sum_all = jnp.concatenate([cache_sum, tail_sum[None]], axis=0)
        out_all = jnp.concatenate([cache_out, tail_out[None]], axis=0)
        top_max = jnp.max(max_all, axis=0, keepdims=True)
        factor = jnp.exp(max_all - top_max)
        total_sum = jnp.sum(sum_all * factor, axis=0)
        merged = jnp.sum(out_all * factor[..., None], axis=0) / total_sum[..., None]
        attn_out = merged.reshape(BATCH_SIZE, Q_HEADS * HEAD_DIM).astype(jnp.bfloat16)
        x_mid = (x_in.astype(jnp.float32) + jnp.dot(attn_out, w_o, preferred_element_type=jnp.float32) + b_o).astype(jnp.bfloat16)
        h_moe = layer_norm(x_mid, ln2_gain, ln2_bias)
        logits = jnp.dot(h_moe, w_router, preferred_element_type=jnp.float32)
        masked = jnp.where(mask_step == 1, logits[:, None, :], NEG_FILL)
        gate_probs = jax.nn.softmax(masked, axis=-1)
        chosen = idx_step[..., None] == jnp.arange(NUM_EXPERTS)[None, None, :]
        gate_mat = jnp.sum(jnp.where(chosen, gate_probs, 0.0), axis=1)

        def expert_body(part_acc, expert_in):
            gate_w, up_w, down_w, gate_col = expert_in
            act_gate = jnp.dot(h_moe, gate_w, preferred_element_type=jnp.float32)
            act_up = jnp.dot(h_moe, up_w, preferred_element_type=jnp.float32)
            mixed_act = (gate_col[:, None] * jax.nn.silu(act_gate) * act_up).astype(jnp.bfloat16)
            blocks = mixed_act.reshape(BATCH_SIZE, KV_GROUP, FF_SHARD).astype(jnp.float32)
            down_blocks = down_w.reshape(KV_GROUP, FF_SHARD, D_MODEL).astype(jnp.float32)
            return part_acc + jnp.einsum('bjf,jfd->bjd', blocks, down_blocks), None

        part_init = jnp.zeros((BATCH_SIZE, KV_GROUP, D_MODEL), jnp.float32)
        part_acc = lax.scan(expert_body, part_init, (w_gate, w_up, w_down, gate_mat.T))[0]
        moe_out = jnp.sum(part_acc.astype(jnp.bfloat16).astype(jnp.float32), axis=1)
        x_out = (x_mid.astype(jnp.float32) + moe_out).astype(jnp.bfloat16)
        return (tail_k, tail_v), x_out

    tail_init = jnp.zeros((BATCH_SIZE, NUM_STEPS, KV_HEADS, HEAD_DIM), jnp.bfloat16)
    final_carry, hidden = lax.scan(decode_step, (tail_init, tail_init), (step_inputs, expert_idx, route_mask, jnp.arange(NUM_STEPS)))
    return hidden, final_carry[0], final_carry[1]
```

```python
import math
import functools
import numpy as np
import jax
import jax.numpy as jnp
from jax import lax
from jax.experimental import pallas as pl
from jax.experimental.pallas import tpu as pltpu
from jax.sharding import PartitionSpec as P

ROPE_BASE = 10000.0
ROPE_MSCALE = math.sqrt(1.0 + math.log(32.0) / math.log(4096.0))
NORM_EPS = 1e-5
NEG_FILL = -1e30
F32 = jnp.float32
BF16 = jnp.bfloat16

NDEV = 8
NB = 16
NS = 3
NR = NS * NB
NQ = NB * 8
DM = 1024
NE = 32
NK = 8
GB = 4
NG = NB // GB

PEERS = ((1, 1, 0), (1, 1, 1), (1, 0, 0), (0, 1, 0), (1, 0, 1), (0, 1, 1), (0, 0, 1))


def nt_dot(a, b):
    return lax.dot_general(a, b, (((1,), (1,)), ((), ())), preferred_element_type=F32)


def dot(a, b):
    return jnp.dot(a, b, preferred_element_type=F32)


def iota(shape, dim):
    return lax.broadcasted_iota(jnp.int32, shape, dim)


def layer_norm(x, gain, bias):
    mean = jnp.mean(x, axis=-1, keepdims=True)
    cen = x - mean
    var = jnp.mean(cen * cen, axis=-1, keepdims=True)
    return (cen * lax.rsqrt(var + NORM_EPS) * gain + bias).astype(BF16)


def lane_gather(x, idx):
    return jnp.take_along_axis(x, idx, axis=1, mode="promise_in_bounds")


def kernel(
    x0_h, xn_h, kt_h, vt_h, len_h, g1_h, b1_h, wq_h, bq_h, wk_h, bk_h, wv_h, bv_h, wo_h, bo_h,
    g2_h, b2_h, wr_h, wg_h, wu_h, wd_h, lf_h, idx_h, mask_h,
    hid_h, tk_h, tv_h,
    xs, kt, vt, lens, g1, b1, wq, bq, wk, bk, wv, bv, wo, bo, g2, b2, wr, wg, wu, wd, lf, idx, mask,
    qz, zs, ks, vs, tail_s, tko, tvo, onehot, us, xm, hido,
    tx1, rx1, rx2, tx3, rx3, rx4,
    dsem, kvsem, osem, ss1, rs1, ss2, rs2, ss3, rs3, ss4, rs4,
):
    me = lax.axis_index("kv")
    my_y, my_x, my_c = me // 4, (me // 2) % 2, me % 2
    peers = [((my_y + y) % 2) * 4 + ((my_x + x) % 2) * 2 + (my_c + c) % 2 for y, x, c in PEERS]

    barrier = pltpu.get_barrier_semaphore()
    for p in peers:
        pl.semaphore_signal(barrier, inc=1, device_id={"kv": p}, device_id_type=pl.DeviceIdType.MESH)

    loads = {}

    def load(name, src, dst):
        c = pltpu.make_async_copy(src, dst, dsem.at[len(loads)])
        c.start()
        loads[name] = c

    load("x0", x0_h, xs.at[pl.ds(0, NB)])
    load("xn", xn_h, xs.at[pl.ds(NB, NR - NB)])
    load("lens", len_h, lens)
    load("lf", lf_h, lf)
    load("g1", g1_h, g1)
    load("b1", b1_h, b1)
    load("wq", wq_h, wq)
    load("wk", wk_h, wk)
    load("wv", wv_h, wv)
    load("bq", bq_h, bq)
    load("bk", bk_h, bk)
    load("bv", bv_h, bv)

    def kv_copy(g, which):
        src, dst = ((kt_h, kt), (vt_h, vt))[which]
        return pltpu.make_async_copy(src.at[pl.ds(g * GB, GB)], dst.at[pl.ds(g * GB, GB)], kvsem.at[g, which])

    for g in range(NG):
        kv_copy(g, 0).start()
        kv_copy(g, 1).start()
    load("idx", idx_h, idx)
    load("mask", mask_h, mask)
    load("wo", wo_h, wo)
    load("bo", bo_h, bo)
    load("g2", g2_h, g2)
    load("b2", b2_h, b2)
    load("wr", wr_h, wr)
    load("wg", wg_h, wg)
    load("wu", wu_h, wu)
    load("wd", wd_h, wd)

    lane1 = iota((1, 128), 1)
    freq = jnp.zeros((1, 128), F32)
    for j in range(32):
        f = float(np.float32(ROPE_BASE) ** np.float32(j * 2.0 / 64))
        freq = jnp.where(lane1 % 32 == j, f, freq)
    loads["lf"].wait()
    loads["lens"].wait()
    lf_row = lf[...]
    inv_freq = 1.0 / (jnp.concatenate([lf_row] * 4, axis=1) * freq)
    pos = jnp.concatenate([jnp.full((8, 128), lens[b], jnp.int32) for b in range(NB)], axis=0)
    pos = pos + iota((NQ, 128), 0) % 4
    angles = pos.astype(F32) * inv_freq
    cos = jnp.cos(angles) * ROPE_MSCALE
    sin = jnp.sin(angles) * ROPE_MSCALE
    lane = iota((NQ, 128), 1)
    half = lane // 64
    low = lane % 64 < 32
    sin = jnp.where(low, -sin, sin)
    g_row = (iota((NQ, 128), 0) // 4) % 2

    for n in ("x0", "xn", "g1", "b1"):
        loads[n].wait()
    h = layer_norm(xs[...].astype(F32), g1[...], b1[...])
    r128 = iota((NQ, NR), 0)
    perm = ((iota((NQ, NR), 1) == (r128 % 4) * NB + r128 // 8) & (r128 % 4 < NS)).astype(F32).astype(BF16)
    h2 = dot(perm, h).astype(BF16)

    for n in ("wq", "wk", "wv", "bq", "bk", "bv"):
        loads[n].wait()
    for c in range(4):
        cols = pl.ds(256 * c, 256)
        q = (dot(h2, wq[:, cols]) + bq[:, cols]).astype(BF16).astype(F32)
        zz = []
        for i in range(2):
            z = q[:, 128 * i:128 * i + 128]
            z = jnp.where(half == g_row, z, pltpu.roll(z, 64, axis=1))
            z = (z * cos + pltpu.roll(z, 32, axis=1) * sin).astype(BF16).astype(F32)
            zs[2 * c + i] = z
            zz.append(jnp.where(half == i, z, 0.0).reshape(NB, 8, 128))
        qz[:, c] = jnp.concatenate(zz, axis=1).astype(BF16)
    for c in range(2):
        cols = pl.ds(256 * c, 256)
        k = (dot(h2, wk[:, cols]) + bk[:, cols]).astype(BF16).astype(F32)
        v = (dot(h2, wv[:, cols]) + bv[:, cols]).astype(BF16).astype(F32)
        for i in range(2):
            z = k[:, 128 * i:128 * i + 128]
            rot = jnp.where(low, pltpu.roll(z, 96, axis=1), pltpu.roll(z, 32, axis=1))
            ks[2 * c + i] = (z * cos + rot * sin).astype(BF16).astype(F32)
            vs[2 * c + i] = v[:, 128 * i:128 * i + 128]

    pl.semaphore_wait(barrier, NDEV - 1)

    def send(src, dst, ssem, rsem, p):
        return pltpu.make_async_remote_copy(
            src_ref=src, dst_ref=dst, send_sem=ssem, recv_sem=rsem,
            device_id={"kv": p}, device_id_type=pl.DeviceIdType.MESH)

    lane8 = iota((8, 128), 1)
    half8 = lane8 // 64
    t_lane = iota((16, 256), 1)
    for h_ in range(8):
        tx1[h_, 8] = jnp.zeros((8, 128), F32)

    def chunk(g, s_tiles):
        return pl.ds(2 * g, s_tiles)

    def attn(g, carry):
        kv_copy(g, 0).wait()
        kv_copy(g, 1).wait()
        outs = []
        mls = [tx1[h_, 8] for h_ in range(8)]
        for i in range(GB):
            b = g * GB + i
            keep = t_lane < lens[b] - me * 256
            per_h = []
            for c in range(4):
                s = dot(qz[b, c], kt[b, pl.ds(128 * c, 128), :]) * 0.125
                s = jnp.where(keep, s, NEG_FILL)
                m = jnp.max(s, axis=1, keepdims=True)
                w = jnp.where(keep, jnp.exp(s - m), 0.0)
                l = jnp.sum(w, axis=1, keepdims=True)
                o = nt_dot(w.astype(BF16), vt[b, pl.ds(128 * c, 128), :])
                for j in range(2):
                    sl = slice(8 * j, 8 * j + 8)
                    hh = 2 * c + j
                    mls[hh] = jnp.where(lane8 == b, m[sl], jnp.where(lane8 == b + NB, l[sl], mls[hh]))
                    per_h.append(o[sl])
            outs.append(per_h)
        for i in range(0, GB, 2):
            for hh in range(8):
                a, b_ = outs[i][hh], outs[i + 1][hh]
                if hh % 2 == 0:
                    b_ = pltpu.roll(b_, 64, axis=1)
                else:
                    a = pltpu.roll(a, 64, axis=1)
                tx1[hh, g * 2 + i // 2] = jnp.where(half8 == 0, a, b_)
        for hh in range(8):
            tx1[hh, 8] = mls[hh]
        return carry

    def send1(n, p, k):
        tiles = pl.ds(2 * n, 2) if n < NG - 1 else pl.ds(2 * n, 3)
        return send(tx1.at[p, tiles], rx1.at[me, tiles], ss1.at[n, k], rs1.at[n, me], p)

    def recv1(n, p, k):
        tiles = pl.ds(2 * n, 2) if n < NG - 1 else pl.ds(2 * n, 3)
        return send(tx1.at[p, tiles], rx1.at[p, tiles], ss1.at[n, k], rs1.at[n, p], p)

    for g in range(NG):
        attn(g, 0)
        for k, p in enumerate(peers):
            send1(g, p, k).start()

    zt = zs[me]
    odd = me % 2
    kcol = ks[me // 2]
    vcol = vs[me // 2]
    kd = jnp.where(half == odd, kcol, pltpu.roll(kcol, 64, axis=1))
    vd = jnp.where(half == odd, vcol, pltpu.roll(vcol, 64, axis=1))
    step8 = iota((8, 128), 0) % 4
    st = [jnp.zeros((8, 128), F32) for _ in range(NS)]
    vroll = []
    for pr in range(NB // 2):
        lo, hi = slice(16 * pr, 16 * pr + 8), slice(16 * pr + 8, 16 * pr + 16)
        zp = jnp.where(half8 == 0, zt[lo], zt[hi])
        kp = jnp.where(half8 == 0, kd[lo], kd[hi])
        vp = jnp.where(half8 == 0, vd[lo], vd[hi])
        vroll.append([vp if d == 0 else pltpu.roll(vp, d, axis=0) for d in range(NS)])
        for d in range(NS):
            prod = zp * (kp if d == 0 else pltpu.roll(kp, d, axis=0))
            s_lo = jnp.sum(jnp.where(half8 == 0, prod, 0.0), axis=1, keepdims=True)
            s_hi = jnp.sum(jnp.where(half8 == 1, prod, 0.0), axis=1, keepdims=True)
            st[d] = jnp.where(lane8 == 2 * pr, s_lo, jnp.where(lane8 == 2 * pr + 1, s_hi, st[d]))
    st = [jnp.where(step8 >= d, st[d] * 0.125, NEG_FILL) for d in range(NS)]
    mt = jnp.maximum(jnp.maximum(st[0], st[1]), st[2])
    wt = [jnp.where(step8 >= d, jnp.exp(st[d] - mt), 0.0) for d in range(NS)]
    lt = wt[0] + wt[1] + wt[2]
    wt = [w.astype(BF16).astype(F32) for w in wt]
    pair_idx = [half8 + 2 * pr for pr in range(NB // 2)]
    ot = []
    for pr in range(NB // 2):
        acc = None
        for d in range(NS):
            term = lane_gather(wt[d], pair_idx[pr]) * vroll[pr][d]
            acc = term if acc is None else acc + term
        ot.append(acc)

    r48 = iota((NR, NQ), 0)
    pick = (iota((NR, NQ), 1) == (r48 // NS) * 8 + r48 % NS).astype(F32).astype(BF16)
    for scr, out, dst, sem in ((ks, tko, tk_h, 0), (vs, tvo, tv_h, 1)):
        for c in range(4):
            rows = dot(pick, scr[c].astype(BF16))
            tail_s[pl.ds(2 * c, NR, stride=8), :] = rows
            tail_s[pl.ds(2 * c + 1, NR, stride=8), :] = pltpu.roll(rows, 64, axis=1)
        out[...] = tail_s[:, :64].astype(BF16)
        pltpu.make_async_copy(out, dst, osem.at[sem]).start()

    loads["idx"].wait()
    loads["mask"].wait()
    diag = iota((NB, NB), 0) == iota((NB, NB), 1)
    lane_e = iota((NR, NE), 1)
    for k in range(NK):
        cols = []
        for s in range(NS):
            row = jnp.broadcast_to(idx[s, k:k + 1, :], (NB, NB))
            cols.append(jnp.sum(jnp.where(diag, row, 0).astype(F32), axis=1, keepdims=True))
        onehot[k] = jnp.where(jnp.concatenate(cols, axis=0).astype(jnp.int32) == lane_e, 1.0, 0.0)

    for t in range(9):
        rx1[me, t] = tx1[me, t]

    for n in ("wo", "bo", "g2", "b2", "wr"):
        loads[n].wait()

    for n in range(NG):
        for k, p in enumerate(peers):
            recv1(n, p, k).wait_recv()
    ml = [rx1[i, 8] for i in range(NDEV)]
    top = mt
    for i in range(NDEV):
        top = jnp.maximum(top, ml[i])
    fac_t = jnp.exp(mt - top)
    fac = [jnp.exp(ml[i] - top) for i in range(NDEV)]
    total = lt * fac_t
    for i in range(NDEV):
        total = total + pltpu.roll(ml[i], 128 - NB, axis=1) * fac[i]
    attn_rows = []
    diag8 = half8 == iota((8, 128), 0) // 4
    for pr in range(NB // 2):
        acc = ot[pr] * lane_gather(fac_t, pair_idx[pr])
        for i in range(NDEV):
            acc = acc + rx1[i, pr] * lane_gather(fac[i], pair_idx[pr])
        acc = acc / lane_gather(total, pair_idx[pr])
        swap = pltpu.roll(pltpu.roll(acc, 64, axis=1), 4, axis=0)
        attn_rows.append(jnp.where(diag8, acc, swap))
    attn_rows = jnp.concatenate(attn_rows, axis=0)
    valid = iota((64, 128), 0) % 4 < NS
    attn_rows = jnp.where(valid, attn_rows, 0.0).astype(BF16)
    r48b = iota((NR, 64), 0)
    pick2 = (iota((NR, 64), 1) == (r48b % NB) * 4 + r48b // NB).astype(F32).astype(BF16)
    rx2[me] = dot(pick2, attn_rows)

    def send2(p, k):
        return send(rx2.at[me], rx2.at[me], ss2.at[k], rs2.at[me], p)

    def recv2(p, k):
        return send(rx2.at[me], rx2.at[p], ss2.at[k], rs2.at[p], p)

    for k, p in enumerate(peers):
        send2(p, k).start()
    for k, p in enumerate(peers):
        recv2(p, k).wait_recv()

    attn_o = jnp.concatenate([rx2[i].astype(BF16) for i in range(NDEV)], axis=1)
    proj = dot(attn_o, wo[...])
    x_mid = (xs[...].astype(F32) + proj + bo[...]).astype(BF16).astype(F32)
    for i in range(NDEV):
        xm[i] = x_mid[:, 128 * i:128 * i + 128]
    h_moe = layer_norm(x_mid, g2[...], b2[...])
    logits = nt_dot(h_moe, wr[...])
    gates = jnp.zeros((NR, NE), F32)
    for k in range(NK):
        on = mask[pl.ds(k, NR, stride=NK), :] == 1
        masked = jnp.where(on, logits, NEG_FILL)
        top_r = jnp.max(masked, axis=1, keepdims=True)
        ex = jnp.exp(masked - top_r)
        den = jnp.sum(ex, axis=1, keepdims=True)
        gates = gates + jnp.where(onehot[k] == 1.0, ex / den, 0.0)
    gates = jnp.concatenate([gates, jnp.zeros((NR, 128 - NE), F32)], axis=1)

    loads["wg"].wait()
    loads["wu"].wait()
    half48 = iota((NR, 128), 1) // 64
    for c in range(8):
        rows = pl.ds(256 * c, 256)
        act = nt_dot(h_moe, wg[rows, :])
        up = nt_dot(h_moe, wu[rows, :])
        gexp = jnp.concatenate([lane_gather(gates, half48 + 4 * c), lane_gather(gates, half48 + 4 * c + 2)], axis=1)
        us[:, rows] = (gexp * (act * (1.0 / (1.0 + jnp.exp(-act)))) * up).astype(BF16)

    loads["wd"].wait()

    def send3(p, k):
        return send(tx3.at[p], rx3.at[me], ss3.at[k], rs3.at[me], p)

    def recv3(p, k):
        return send(tx3.at[p], rx3.at[p], ss3.at[k], rs3.at[p], p)

    u_all = us[...]
    for y, x in ((1, 1), (1, 0), (0, 1), (0, 0)):
        chip = ((my_y + y) % 2) * 2 + (my_x + x) % 2
        part = dot(u_all, wd[:, pl.ds(pl.multiple_of(256 * chip, 256), 256)]).astype(BF16).astype(F32)
        tx3[2 * chip] = part[:, :128]
        tx3[2 * chip + 1] = part[:, 128:]
        for k, (p, off) in enumerate(zip(peers, PEERS)):
            if off[:2] == (y, x):
                send3(p, k).start()
    y_acc = tx3[me]
    for k, p in enumerate(peers):
        recv3(p, k).wait_recv()
        y_acc = y_acc + rx3[p]
    rx4[me] = (xm[me] + y_acc).astype(BF16).astype(F32)

    def send4(p, k):
        return send(rx4.at[me], rx4.at[me], ss4.at[k], rs4.at[me], p)

    def recv4(p, k):
        return send(rx4.at[me], rx4.at[p], ss4.at[k], rs4.at[p], p)

    for k, p in enumerate(peers):
        send4(p, k).start()
    for k, p in enumerate(peers):
        recv4(p, k).wait_recv()
    for i in range(NDEV):
        hido[:, pl.ds(128 * i, 128)] = rx4[i].astype(BF16)
    pltpu.make_async_copy(hido, hid_h, osem.at[2]).start()

    for k, p in enumerate(peers):
        for n in range(NG):
            send1(n, p, k).wait_send()
        send2(p, k).wait_send()
        send3(p, k).wait_send()
        send4(p, k).wait_send()
    pltpu.make_async_copy(tko, tk_h, osem.at[0]).wait()
    pltpu.make_async_copy(tvo, tv_h, osem.at[1]).wait()
    pltpu.make_async_copy(hido, hid_h, osem.at[2]).wait()


def solution(mesh):
    def layer_steps(x_first, next_emb, k_cache, v_cache, seq_len, ln1_gain, ln1_bias, w_q, b_q, w_k, b_k, w_v, b_v, w_o, b_o, ln2_gain, ln2_bias, w_router, w_gate, w_up, w_down, long_factor, expert_idx, route_mask):
        row = lambda a: a.reshape(1, -1)
        args = (
            x_first, next_emb.reshape(NR - NB, DM),
            k_cache.transpose(0, 2, 3, 1).reshape(NB, 512, 256),
            v_cache.transpose(0, 2, 3, 1).reshape(NB, 512, 256),
            seq_len, row(ln1_gain), row(ln1_bias), w_q, row(b_q), w_k, row(b_k), w_v, row(b_v), w_o, row(b_o),
            row(ln2_gain), row(ln2_bias), w_router.T,
            w_gate.transpose(0, 2, 1).reshape(2048, DM), w_up.transpose(0, 2, 1).reshape(2048, DM),
            w_down.reshape(2048, DM), row(long_factor),
            expert_idx.transpose(0, 2, 1), route_mask.reshape(NR * NK, NE),
        )
        vm = lambda shape, dt=F32: pltpu.VMEM(shape, dt)
        dma = lambda shape: pltpu.SemaphoreType.DMA(shape)
        scratch = [
            vm((NR, DM), BF16), vm((NB, 512, 256), BF16), vm((NB, 512, 256), BF16), pltpu.SMEM((NB,), jnp.int32),
            vm((1, DM)), vm((1, DM)), vm((DM, DM), BF16), vm((1, DM)), vm((DM, 512), BF16), vm((1, 512)),
            vm((DM, 512), BF16), vm((1, 512)), vm((DM, DM), BF16), vm((1, DM)), vm((1, DM)), vm((1, DM)),
            vm((NE, DM), BF16), vm((2048, DM), BF16), vm((2048, DM), BF16), vm((2048, DM), BF16),
            vm((1, 32)), vm((NS, NK, NB), jnp.int32), vm((NR * NK, NE), jnp.int32),
            vm((NB, 4, 16, 128), BF16), vm((8, NQ, 128)), vm((4, NQ, 128)), vm((4, NQ, 128)),
            vm((NR * 8, 128)), vm((NR * 8, 64), BF16), vm((NR * 8, 64), BF16), vm((NK, NR, NE)),
            vm((NR, 2048), BF16), vm((8, NR, 128)), vm((NR, DM), BF16),
            vm((8, 9, 8, 128)), vm((8, 9, 8, 128)), vm((8, NR, 128)), vm((8, NR, 128)), vm((8, NR, 128)), vm((8, NR, 128)),
            dma((22,)), dma((NG, 2)), dma((3,)),
            dma((NG, 7)), dma((NG, 8)), dma((7,)), dma((8,)), dma((7,)), dma((8,)), dma((7,)), dma((8,)),
        ]
        hbm = pl.BlockSpec(memory_space=pl.ANY)
        hid, tk, tv = pl.pallas_call(
            kernel,
            out_shape=(
                jax.ShapeDtypeStruct((NR, DM), BF16),
                jax.ShapeDtypeStruct((NR * 8, 64), BF16),
                jax.ShapeDtypeStruct((NR * 8, 64), BF16),
            ),
            in_specs=[hbm] * len(args),
            out_specs=(hbm,) * 3,
            scratch_shapes=scratch,
            compiler_params=pltpu.CompilerParams(
                collective_id=0, has_side_effects=True, vmem_limit_bytes=67043328),
        )(*args)
        return hid.reshape(NS, NB, DM), tk.reshape(NB, NS, 8, 64), tv.reshape(NB, NS, 8, 64)

    replicated = P()
    in_specs = (P('dp'), P(None, 'dp'), P('dp', 'kv'), P('dp', 'kv'), P('dp')) + (replicated,) * 13 + (P(None, None, 'kv'), P(None, None, 'kv'), P(None, 'kv'), replicated, P(None, 'dp'), P(None, 'dp'))
    out_specs = (P(None, 'dp'), P('dp'), P('dp'))
    return jax.shard_map(layer_steps, mesh=mesh, in_specs=in_specs, out_specs=out_specs, check_vma=False)
```
